32 devices in a mesh: replica: 2 (over core), model: 4 (over y, x), copy: 4 (over z).
Axes of the slice: x: 2, y: 2, z: 4, core: 2. Of those that a mesh axis runs over, the one named last changes fastest.
Arguments:
- slope_up: bfloat16 [8, 1280, 5120], P(('copy', 'replica'), None, 'model'), parts along dimension 0, may hold values from -0.875 to 0.875
- slope_down: bfloat16 [8, 5120, 1280], P(('copy', 'replica'), 'model'), parts along dimension 0, may hold values from -0.875 to 0.875
- slope_norm: bfloat16 [8, 1280], P(('copy', 'replica')), parts along dimension 0, may hold values from -8 to 8
- param_up: float32 [5120, 5120], P(('copy', 'replica'), 'model'), parts along dimension 0, may hold values from -0.25 to 0.25
- param_down: float32 [20480, 1280], P(('copy', 'model'), 'replica'), parts along dimension 0, may hold values from -0.125 to 0.125
- param_norm: float32 [5120], P(('copy', 'replica')), parts along dimension 0, may hold values from 0.25 to 1.75
Outputs:
- half_up: bfloat16 [5120, 5120], P('copy', 'model'), parts along dimension 0
- half_down: bfloat16 [20480, 1280], P(('copy', 'model')), parts along dimension 0
- half_norm: bfloat16 [5120], P('copy'), parts along dimension 0
- next_up: float32 [5120, 5120], P(('copy', 'replica'), 'model'), parts along dimension 0
- next_down: float32 [20480, 1280], P(('copy', 'model'), 'replica'), parts along dimension 0
- next_norm: float32 [5120], P(('copy', 'replica')), parts along dimension 0
The draws below stay inside these ranges and needn't reach their ends.
There are 4 independent parts, one for each index of `copy`. The reference program is written for one: setup_inputs(seed, part) draws one part's arguments, and reference() takes and returns one part's arrays. A program takes and returns all parts, laid end to end along the dimension named above; each array names one. Nothing has to cross between parts.
All inputs are finite; a program needn't handle non-finite values.
Results may differ from the reference program's by a relative error of at most 0.011.
Values may be sent and summed in bfloat16 or wider, within the bound.
A program may use at most 128 MiB of HBM per device.

```python
import jax
import jax.numpy as jnp
from jax import lax

WIDTH = 1280
INNER = 5120
REPLICAS = 2


def spiked(drawn, rng, source, target, shards_of, factor):
    def block_of(dim):
        return (jnp.arange(drawn.shape[dim]) // (drawn.shape[dim] // shards_of)).reshape((-1,) + (1,) * (drawn.ndim - 1 - dim))

    first = jax.random.permutation(rng, shards_of)[block_of(target)]
    other_side = (block_of(target) + shards_of // 2) % shards_of
    return jnp.where((block_of(source) == first) | (block_of(source) == other_side), factor * drawn, drawn)


def level_of(stream_key, shape, cuts, least, top_value):
    level = 1.0
    for dim, parts in cuts:
        steps = jax.random.uniform(jax.random.fold_in(jax.random.fold_in(stream_key, 6), dim), (parts,), jnp.float32, least / len(cuts), top_value / len(cuts))
        level = level * jnp.repeat(jnp.exp(steps), shape[dim] // parts).reshape((-1,) + (1,) * (len(shape) - 1 - dim))
    return level


def noise_with(own_key, dims, spread, limit, pieces, heavy, dtype=jnp.bfloat16):
    array = spread * jax.random.normal(own_key, dims, jnp.float32)
    if pieces:
        array = array * level_of(own_key, dims, pieces, -0.22, 0.18)
    return jnp.clip(spiked(array, jax.random.fold_in(own_key, 3), *heavy), -limit, limit).astype(dtype)


def setup_inputs(seed: int = 0, part: int = 0) -> dict:
    key_of = jax.random.split(jax.random.key(seed), 7)
    part_keys = jax.random.split(jax.random.fold_in(key_of[6], part), 7)
    return {
        "slope_up": noise_with(part_keys[0], (REPLICAS, WIDTH, INNER), 0.1, 0.875, ((0, 2), (2, 4)), (0, 1, 2, 2.0)),
        "slope_down": noise_with(part_keys[1], (REPLICAS, INNER, WIDTH), 0.1, 0.875, ((0, 2), (1, 4)), (0, 2, 2, 2.0)),
        "slope_norm": noise_with(part_keys[2], (REPLICAS, WIDTH), 1.0, 8.0, ((0, 2),), (0, 1, 2, 2.0)),
        "param_up": noise_with(part_keys[3], (WIDTH, INNER), WIDTH ** -0.5, 0.25, ((0, 2), (1, 4)), (1, 0, 4, 2.0), jnp.float32),
        "param_down": noise_with(part_keys[4], (INNER, WIDTH), INNER ** -0.5, 0.125, ((0, 4), (1, 2)), (0, 1, 4, 2.0), jnp.float32),
        "param_norm": jnp.clip(1.0 + 0.15 * jax.random.normal(part_keys[5], (WIDTH,), jnp.float32), 0.25, 1.75),
    }


learn_rate = 0.5

def reference(slope_up, slope_down, slope_norm, param_up, param_down, param_norm):
    mean_up = lax.optimization_barrier(jnp.sum(slope_up.astype(jnp.float32), axis=0)) * REPLICAS ** (-0.5)
    mean_down = lax.optimization_barrier(jnp.sum(slope_down.astype(jnp.float32), axis=0)) * REPLICAS ** (-0.5)
    mean_norm = lax.optimization_barrier(jnp.sum(slope_norm.astype(jnp.float32), axis=0)) * REPLICAS ** (-0.5)
    ratio_up = jnp.sqrt(lax.optimization_barrier(jnp.sum(param_up * param_up, axis=1, keepdims=True))) * lax.rsqrt(lax.optimization_barrier(jnp.sum(mean_up * mean_up, axis=1, keepdims=True)) + 1e-06)
    mean_up = mean_up * ratio_up
    ratio_down = jnp.sqrt(lax.optimization_barrier(jnp.sum(param_down * param_down, axis=0, keepdims=True))) * lax.rsqrt(lax.optimization_barrier(jnp.sum(mean_down * mean_down, axis=0, keepdims=True)) + 1e-06)
    mean_down = mean_down * ratio_down
    next_up = param_up - learn_rate * mean_up
    next_down = param_down - learn_rate * mean_down
    next_norm = param_norm - learn_rate * mean_norm
    half_up = next_up.astype(jnp.bfloat16)
    half_down = next_down.astype(jnp.bfloat16)
    half_norm = next_norm.astype(jnp.bfloat16)
    return (half_up, half_down, half_norm, next_up, next_down, next_norm)
```

```python
import functools

import jax
import jax.numpy as jnp
from jax import lax
from jax.experimental import pallas as pl
from jax.experimental.pallas import tpu as pltpu
from jax.sharding import PartitionSpec as P

learn_rate = 0.5


def shards(slope_up, slope_down, slope_norm, param_up, param_down, param_norm):
    mean_up, mean_down = (
        lax.psum_scatter(
            slope_up[0].astype(jnp.float32).astype(jnp.bfloat16),
            "replica",
            scatter_dimension=0,
            tiled=True,
        ).astype(jnp.float32),
        lax.psum_scatter(
            slope_down[0].astype(jnp.float32).astype(jnp.bfloat16),
            "replica",
            scatter_dimension=1,
            tiled=True,
        ).astype(jnp.float32),
    )
    whole_norm = lax.psum(slope_norm[0].astype(jnp.float32), "replica")
    place = lax.axis_index("replica")
    mean_norm = lax.dynamic_slice_in_dim(
        whole_norm, place * param_norm.shape[0], param_norm.shape[0]
    )
    mean_rate = lax.axis_size("replica") ** (-0.5)
    mean_up = mean_up * mean_rate
    mean_down = mean_down * mean_rate
    mean_norm = mean_norm * mean_rate
    own_up, own_down, slope_up_norm, slope_down_norm = lax.psum(
        (
            jnp.sum(param_up * param_up, axis=1, keepdims=True),
            jnp.sum(param_down * param_down, axis=0, keepdims=True),
            jnp.sum(mean_up * mean_up, axis=1, keepdims=True),
            jnp.sum(mean_down * mean_down, axis=0, keepdims=True),
        ),
        "model",
    )
    mean_up = mean_up * (jnp.sqrt(own_up) * lax.rsqrt(slope_up_norm + 1e-06))
    mean_down = mean_down * (jnp.sqrt(own_down) * lax.rsqrt(slope_down_norm + 1e-06))
    next_up = param_up - learn_rate * mean_up
    next_down = param_down - learn_rate * mean_down
    next_norm = param_norm - learn_rate * mean_norm
    half_up, half_down, half_norm = (
        lax.all_gather(next_up.astype(jnp.bfloat16), "replica", axis=0, tiled=True),
        lax.all_gather(next_down.astype(jnp.bfloat16), "replica", axis=1, tiled=True),
        lax.all_gather(next_norm.astype(jnp.bfloat16), "replica", axis=0, tiled=True),
    )
    return (half_up, half_down, half_norm, next_up, next_down, next_norm)


MESH = pl.DeviceIdType.MESH
LANES = 128
ROWS = 32


def update_kernel(
    replicas,
    models,
    slope_up,
    slope_down,
    slope_norm,
    param_up,
    param_down,
    param_norm,
    half_up,
    half_down,
    half_norm,
    next_up,
    next_down,
    next_norm,
    own_up,
    peer_up,
    own_down,
    peer_down,
    own_vec,
    peer_vec,
    peer_gain,
    sum_vec,
    whole_vec,
    part,
    got,
    square,
    spread,
    load_sem,
    pair_send,
    pair_recv,
    norm_send,
    norm_recv,
):
    me = lax.axis_index("replica")
    other = 1 - me
    spot = lax.axis_index("model")
    share, inner = param_up.shape
    depth = param_down.shape[0]
    up_chunks = share // LANES
    down_rows = 256 if depth % 256 == 0 else LANES
    down_chunks = depth // down_rows
    mine = pl.multiple_of(me * share, LANES)
    theirs = pl.multiple_of(other * share, LANES)
    rate = replicas ** (-0.5)
    f32 = jnp.float32

    loads = {}

    def load(name, source, target):
        copy = pltpu.make_async_copy(source, target, load_sem.at[len(loads)])
        copy.start()
        loads[name] = copy

    pairs = {}

    def push(name, source, target):
        copy = pltpu.make_async_remote_copy(
            source,
            target,
            pair_send.at[len(pairs)],
            pair_recv.at[len(pairs)],
            device_id={"replica": other},
            device_id_type=MESH,
        )
        copy.start()
        pairs[name] = copy

    def up_rows(c):
        return pl.ds(c * LANES, LANES)

    def down_part(c):
        return pl.ds(c * down_rows, down_rows)

    load("pu", param_up, next_up)
    load("pd", param_down, next_down)
    for c in range(up_chunks):
        load(
            ("up", c),
            slope_up.at[0, pl.ds(mine + c * LANES, LANES), :],
            own_up.at[up_rows(c), :],
        )
    for c in range(down_chunks):
        load(
            ("down", c),
            slope_down.at[0, down_part(c), pl.ds(mine, share)],
            own_down.at[down_part(c), :],
        )
    load("sn", slope_norm, own_vec)

    barrier = pltpu.get_barrier_semaphore()
    pl.semaphore_signal(
        barrier, inc=1, device_id={"replica": other}, device_id_type=MESH
    )
    for k in range(1, models):
        pl.semaphore_signal(
            barrier,
            inc=1,
            device_id={"model": lax.rem(spot + k, models)},
            device_id_type=MESH,
        )
    pl.semaphore_wait(barrier, models)

    for c in range(up_chunks):
        push(
            ("up", c),
            slope_up.at[0, pl.ds(theirs + c * LANES, LANES), :],
            peer_up.at[up_rows(c), :],
        )
    for c in range(down_chunks):
        push(
            ("down", c),
            slope_down.at[0, down_part(c), pl.ds(theirs, share)],
            peer_down.at[down_part(c), :],
        )
    push("sn", slope_norm, peer_vec)
    push("pn", param_norm, peer_gain)

    sent = []

    def share_norm(i):
        for k in range(1, models):
            copy = pltpu.make_async_remote_copy(
                part.at[i],
                got.at[i, k - 1],
                norm_send.at[i, k - 1],
                norm_recv.at[i, k - 1],
                device_id={"model": lax.rem(spot + k, models)},
                device_id_type=MESH,
            )
            copy.start()
            sent.append((i, copy))

    def whole_norm(i):
        total = part[i]
        for j, copy in sent:
            if j == i:
                copy.wait_recv()
        for k in range(1, models):
            total = total + got[i, k - 1]
        return total

    def row_squares(i, c, value):
        @pl.loop(0, LANES // ROWS)
        def _(r):
            rows = pl.ds(c * LANES + r * ROWS, ROWS)
            total = jnp.zeros((ROWS, LANES), f32)
            for j in range(inner // LANES):
                x = value(rows, pl.ds(j * LANES, LANES))
                total = total + x * x
            square[pl.ds(r * ROWS, ROWS), :] = total

        part[i, :, c * LANES : (c + 1) * LANES] = jnp.sum(
            square[...].T, axis=0, keepdims=True
        )

    def column_squares(c, value, totals):
        def body(r, totals):
            rows = pl.ds(c * down_rows + r * ROWS, ROWS)
            out = []
            for j, total in enumerate(totals):
                x = value(rows, pl.ds(j * LANES, LANES))
                x = x * x
                for s in range(ROWS // 8):
                    total = total + x[s * 8 : (s + 1) * 8]
                out.append(total)
            return tuple(out)

        return lax.fori_loop(0, down_rows // ROWS, body, totals)

    def zeros():
        return tuple(jnp.zeros((8, LANES), f32) for _ in range(share // LANES))

    def put_columns(i, totals):
        for j, total in enumerate(totals):
            part[i, :, j * LANES : (j + 1) * LANES] = jnp.sum(
                total, axis=0, keepdims=True
            )

    def sum_up(rows, lanes):
        return own_up[rows, lanes].astype(f32) + peer_up[rows, lanes].astype(f32)

    def sum_down(rows, lanes):
        return own_down[rows, lanes].astype(f32) + peer_down[rows, lanes].astype(f32)

    loads["pu"].wait()
    for c in range(up_chunks):
        row_squares(0, c, lambda rows, lanes: next_up[rows, lanes])
    share_norm(0)
    loads["pd"].wait()
    totals = zeros()
    for c in range(down_chunks):
        totals = column_squares(c, lambda rows, lanes: next_down[rows, lanes], totals)
    put_columns(1, totals)
    share_norm(1)

    for c in range(up_chunks):
        loads["up", c].wait()
        pairs["up", c].wait_recv()
        row_squares(2, c, lambda rows, lanes: sum_up(rows, lanes) * rate)
    share_norm(2)

    totals = zeros()
    for c in range(down_chunks):
        loads["down", c].wait()
        pairs["down", c].wait_recv()
        totals = column_squares(
            c, lambda rows, lanes: sum_down(rows, lanes) * rate, totals
        )
    put_columns(3, totals)
    share_norm(3)

    loads["sn"].wait()
    pairs["sn"].wait_recv()
    pairs["pn"].wait_recv()
    sum_vec[...] = (
        (own_vec[...].astype(f32) + peer_vec[...].astype(f32)) * rate * learn_rate
    )
    new_gain = param_norm[...] - sum_vec[:, pl.ds(mine, share)]
    next_norm[...] = new_gain
    whole_vec[:, pl.ds(mine, share)] = new_gain
    whole_vec[:, pl.ds(theirs, share)] = (
        peer_gain[...] - sum_vec[:, pl.ds(theirs, share)]
    )
    half_norm[...] = whole_vec[...].astype(jnp.bfloat16)

    ratio = jnp.sqrt(whole_norm(0)) * lax.rsqrt(whole_norm(2) + 1e-06)
    ratio = ratio * (rate * learn_rate)
    for c in range(up_chunks):
        spread[...] = jnp.broadcast_to(
            ratio[:, c * LANES : (c + 1) * LANES], (LANES, LANES)
        ).T

        @pl.loop(0, LANES // ROWS)
        def _(r):
            rows = pl.ds(c * LANES + r * ROWS, ROWS)
            scale = spread[pl.ds(r * ROWS, ROWS), :]
            for j in range(inner // LANES):
                lanes = pl.ds(j * LANES, LANES)
                new = next_up[rows, lanes] - sum_up(rows, lanes) * scale
                next_up[rows, lanes] = new
                half_up[pl.ds(mine + c * LANES + r * ROWS, ROWS), lanes] = new.astype(
                    jnp.bfloat16
                )

        block = half_up.at[pl.ds(mine + c * LANES, LANES), :]
        push(("half_up", c), block, block)

    ratio = jnp.sqrt(whole_norm(1)) * lax.rsqrt(whole_norm(3) + 1e-06)
    ratio = ratio * (rate * learn_rate)
    scales = [
        jnp.broadcast_to(ratio[:, j * LANES : (j + 1) * LANES], (ROWS, LANES))
        for j in range(share // LANES)
    ]
    for c in range(down_chunks):

        @pl.loop(0, down_rows // ROWS)
        def _(r):
            rows = pl.ds(c * down_rows + r * ROWS, ROWS)
            for j, scale in enumerate(scales):
                lanes = pl.ds(j * LANES, LANES)
                new = next_down[rows, lanes] - sum_down(rows, lanes) * scale
                next_down[rows, lanes] = new
                half_down[rows, pl.ds(mine + j * LANES, LANES)] = new.astype(
                    jnp.bfloat16
                )

        block = half_down.at[down_part(c), pl.ds(mine, share)]
        push(("half_down", c), block, block)

    for name, copy in pairs.items():
        copy.wait_send()
        if name[0] in ("half_up", "half_down"):
            copy.wait_recv()
    for _, copy in sent:
        copy.wait_send()


def fused(replicas, models, slope_up, slope_down, slope_norm, param_up, param_down, param_norm):
    share, inner = param_up.shape
    depth = param_down.shape[0]
    width = slope_up.shape[1]
    down_chunks = depth // (256 if depth % 256 == 0 else LANES)
    up_chunks = share // LANES
    moves = up_chunks + down_chunks + 2
    bf16, f32 = jnp.bfloat16, jnp.float32
    hbm = pl.BlockSpec(memory_space=pltpu.HBM)
    vmem = pl.BlockSpec(memory_space=pltpu.VMEM)
    outs = pl.pallas_call(
        functools.partial(update_kernel, replicas, models),
        out_shape=(
            OUT((width, inner), bf16),
            OUT((depth, width), bf16),
            OUT((1, width), bf16),
            OUT((share, inner), f32),
            OUT((depth, share), f32),
            OUT((1, share), f32),
        ),
        in_specs=[hbm] * 5 + [vmem],
        out_specs=(vmem,) * 6,
        scratch_shapes=[
            pltpu.VMEM((share, inner), bf16),
            pltpu.VMEM((share, inner), bf16),
            pltpu.VMEM((depth, share), bf16),
            pltpu.VMEM((depth, share), bf16),
            pltpu.VMEM((1, width), bf16),
            pltpu.VMEM((1, width), bf16),
            pltpu.VMEM((1, share), f32),
            pltpu.VMEM((1, width), f32),
            pltpu.VMEM((1, width), f32),
            pltpu.VMEM((4, 1, share), f32),
            pltpu.VMEM((4, models - 1, 1, share), f32),
            pltpu.VMEM((LANES, LANES), f32),
            pltpu.VMEM((LANES, LANES), f32),
            pltpu.SemaphoreType.DMA((moves + 1,)),
            pltpu.SemaphoreType.DMA((2 * moves,)),
            pltpu.SemaphoreType.DMA((2 * moves,)),
            pltpu.SemaphoreType.DMA((4, models - 1)),
            pltpu.SemaphoreType.DMA((4, models - 1)),
        ],
        compiler_params=pltpu.CompilerParams(
            collective_id=0, has_side_effects=True, vmem_limit_bytes=24 * 2**20
        ),
    )(
        *(
            pltpu.with_memory_space_constraint(x, pltpu.HBM)
            for x in (slope_up, slope_down, slope_norm, param_up, param_down)
        ),
        param_norm[None],
    )
    half_up, half_down, half_norm, next_up, next_down, next_norm = outs
    return half_up, half_down, half_norm[0], next_up, next_down, next_norm[0]


def suits(mesh, *arrays):
    slope_up, param_up, param_down = arrays
    return (
        mesh.shape["replica"] == 2
        and mesh.shape["model"] > 1
        and param_up.shape[0] % LANES == 0
        and param_up.shape[1] % LANES == 0
        and param_down.shape[0] % LANES == 0
    )


def step(mesh, slope_up, slope_down, slope_norm, param_up, param_down, param_norm):
    args = (slope_up, slope_down, slope_norm, param_up, param_down, param_norm)
    if suits(mesh, slope_up, param_up, param_down):
        return fused(mesh.shape["replica"], mesh.shape["model"], *args)
    return shards(*args)


OUT = pltpu.VMEM


def solution(mesh):
    return jax.shard_map(
        functools.partial(step, mesh),
        mesh=mesh,
        in_specs=(
            P(("copy", "replica"), None, "model"),
            P(("copy", "replica"), "model", None),
            P(("copy", "replica"), None),
            P(("copy", "replica"), "model"),
            P(("copy", "model"), "replica"),
            P(("copy", "replica")),
        ),
        out_specs=(
            P("copy", "model"),
            P(("copy", "model"), None),
            P("copy"),
            P(("copy", "replica"), "model"),
            P(("copy", "model"), "replica"),
            P(("copy", "replica")),
        ),
        check_vma=False,
    )
```

```python
import functools

import jax
import jax.numpy as jnp
from jax import lax
from jax.experimental import pallas as pl
from jax.experimental.pallas import tpu as pltpu
from jax.sharding import PartitionSpec as P

learn_rate = 0.5


def shards(slope_up, slope_down, slope_norm, param_up, param_down, param_norm):
    mean_up, mean_down = (
        lax.psum_scatter(
            slope_up[0].astype(jnp.float32).astype(jnp.bfloat16),
            "replica",
            scatter_dimension=0,
            tiled=True,
        ).astype(jnp.float32),
        lax.psum_scatter(
            slope_down[0].astype(jnp.float32).astype(jnp.bfloat16),
            "replica",
            scatter_dimension=1,
            tiled=True,
        ).astype(jnp.float32),
    )
    whole_norm = lax.psum(slope_norm[0].astype(jnp.float32), "replica")
    place = lax.axis_index("replica")
    mean_norm = lax.dynamic_slice_in_dim(
        whole_norm, place * param_norm.shape[0], param_norm.shape[0]
    )
    mean_rate = lax.axis_size("replica") ** (-0.5)
    mean_up = mean_up * mean_rate
    mean_down = mean_down * mean_rate
    mean_norm = mean_norm * mean_rate
    own_up, own_down, slope_up_norm, slope_down_norm = lax.psum(
        (
            jnp.sum(param_up * param_up, axis=1, keepdims=True),
            jnp.sum(param_down * param_down, axis=0, keepdims=True),
            jnp.sum(mean_up * mean_up, axis=1, keepdims=True),
            jnp.sum(mean_down * mean_down, axis=0, keepdims=True),
        ),
        "model",
    )
    mean_up = mean_up * (jnp.sqrt(own_up) * lax.rsqrt(slope_up_norm + 1e-06))
    mean_down = mean_down * (jnp.sqrt(own_down) * lax.rsqrt(slope_down_norm + 1e-06))
    next_up = param_up - learn_rate * mean_up
    next_down = param_down - learn_rate * mean_down
    next_norm = param_norm - learn_rate * mean_norm
    half_up, half_down, half_norm = (
        lax.all_gather(next_up.astype(jnp.bfloat16), "replica", axis=0, tiled=True),
        lax.all_gather(next_down.astype(jnp.bfloat16), "replica", axis=1, tiled=True),
        lax.all_gather(next_norm.astype(jnp.bfloat16), "replica", axis=0, tiled=True),
    )
    return (half_up, half_down, half_norm, next_up, next_down, next_norm)


MESH = pl.DeviceIdType.MESH
LANES = 128
ROWS = 32


def update_kernel(
    replicas,
    models,
    slope_up,
    slope_down,
    slope_norm,
    param_up,
    param_down,
    param_norm,
    half_up,
    half_down,
    half_norm,
    next_up,
    next_down,
    next_norm,
    own_up,
    peer_up,
    own_down,
    peer_down,
    own_vec,
    peer_vec,
    own_gain,
    peer_gain,
    sum_vec,
    part,
    got,
    square,
    spread,
    load_sem,
    pair_send,
    pair_recv,
    norm_send,
    norm_recv,
):
    me = lax.axis_index("replica")
    other = 1 - me
    spot = lax.axis_index("model")
    share, inner = param_up.shape
    depth = param_down.shape[0]
    up_chunks = share // LANES
    down_rows = 256 if depth % 256 == 0 else LANES
    down_chunks = depth // down_rows
    mine = pl.multiple_of(me * share, LANES)
    theirs = pl.multiple_of(other * share, LANES)
    rate = replicas ** (-0.5)
    f32 = jnp.float32

    loads = {}

    def load(name, source, target):
        copy = pltpu.make_async_copy(source, target, load_sem.at[len(loads)])
        copy.start()
        loads[name] = copy

    pairs = {}

    def push(name, source, target):
        copy = pltpu.make_async_remote_copy(
            source,
            target,
            pair_send.at[len(pairs)],
            pair_recv.at[len(pairs)],
            device_id={"replica": other},
            device_id_type=MESH,
        )
        copy.start()
        pairs[name] = copy

    def up_rows(c):
        return pl.ds(c * LANES, LANES)

    def down_part(c):
        return pl.ds(c * down_rows, down_rows)

    load("pu", param_up, next_up)
    load("pd", param_down, next_down)
    for c in range(up_chunks):
        load(
            ("up", c),
            slope_up.at[0, pl.ds(mine + c * LANES, LANES), :],
            own_up.at[up_rows(c), :],
        )
    for c in range(down_chunks):
        load(
            ("down", c),
            slope_down.at[0, down_part(c), pl.ds(mine, share)],
            own_down.at[down_part(c), :],
        )
    load("sn", slope_norm, own_vec)
    load("pn", param_norm, own_gain)

    barrier = pltpu.get_barrier_semaphore()
    pl.semaphore_signal(
        barrier, inc=1, device_id={"replica": other}, device_id_type=MESH
    )
    for k in range(1, models):
        pl.semaphore_signal(
            barrier,
            inc=1,
            device_id={"model": lax.rem(spot + k, models)},
            device_id_type=MESH,
        )
    pl.semaphore_wait(barrier, models)

    for c in range(up_chunks):
        push(
            ("up", c),
            slope_up.at[0, pl.ds(theirs + c * LANES, LANES), :],
            peer_up.at[up_rows(c), :],
        )
    for c in range(down_chunks):
        push(
            ("down", c),
            slope_down.at[0, down_part(c), pl.ds(theirs, share)],
            peer_down.at[down_part(c), :],
        )
    push("sn", slope_norm, peer_vec)
    push("pn", param_norm, peer_gain)

    sent = []

    def share_norm(i):
        for k in range(1, models):
            copy = pltpu.make_async_remote_copy(
                part.at[i],
                got.at[i, k - 1],
                norm_send.at[i, k - 1],
                norm_recv.at[i, k - 1],
                device_id={"model": lax.rem(spot + k, models)},
                device_id_type=MESH,
            )
            copy.start()
            sent.append((i, copy))

    def whole_norm(i):
        total = part[i]
        for j, copy in sent:
            if j == i:
                copy.wait_recv()
        for k in range(1, models):
            total = total + got[i, k - 1]
        return total

    def row_squares(i, c, value):
        @pl.loop(0, LANES // ROWS)
        def _(r):
            rows = pl.ds(c * LANES + r * ROWS, ROWS)
            total = jnp.zeros((ROWS, LANES), f32)
            for j in range(inner // LANES):
                x = value(rows, pl.ds(j * LANES, LANES))
                total = total + x * x
            square[pl.ds(r * ROWS, ROWS), :] = total

        part[i, :, c * LANES : (c + 1) * LANES] = jnp.sum(
            square[...].T, axis=0, keepdims=True
        )

    def column_squares(c, value, totals):
        def body(r, totals):
            rows = pl.ds(c * down_rows + r * ROWS, ROWS)
            out = []
            for j, total in enumerate(totals):
                x = value(rows, pl.ds(j * LANES, LANES))
                x = x * x
                for s in range(ROWS // 8):
                    total = total + x[s * 8 : (s + 1) * 8]
                out.append(total)
            return tuple(out)

        return lax.fori_loop(0, down_rows // ROWS, body, totals)

    def zeros():
        return tuple(jnp.zeros((8, LANES), f32) for _ in range(share // LANES))

    def put_columns(i, totals):
        for j, total in enumerate(totals):
            part[i, :, j * LANES : (j + 1) * LANES] = jnp.sum(
                total, axis=0, keepdims=True
            )

    def sum_up(rows, lanes):
        return own_up[rows, lanes].astype(f32) + peer_up[rows, lanes].astype(f32)

    def sum_down(rows, lanes):
        return own_down[rows, lanes].astype(f32) + peer_down[rows, lanes].astype(f32)

    loads["pu"].wait()
    for c in range(up_chunks):
        row_squares(0, c, lambda rows, lanes: next_up[rows, lanes])
    share_norm(0)
    loads["pd"].wait()
    totals = zeros()
    for c in range(down_chunks):
        totals = column_squares(c, lambda rows, lanes: next_down[rows, lanes], totals)
    put_columns(1, totals)
    share_norm(1)

    for c in range(up_chunks):
        loads["up", c].wait()
        pairs["up", c].wait_recv()
        row_squares(2, c, lambda rows, lanes: sum_up(rows, lanes) * rate)
    share_norm(2)

    totals = zeros()
    for c in range(down_chunks):
        loads["down", c].wait()
        pairs["down", c].wait_recv()
        totals = column_squares(
            c, lambda rows, lanes: sum_down(rows, lanes) * rate, totals
        )
    put_columns(3, totals)
    share_norm(3)

    loads["sn"].wait()
    loads["pn"].wait()
    pairs["sn"].wait_recv()
    pairs["pn"].wait_recv()
    sum_vec[...] = (
        (own_vec[...].astype(f32) + peer_vec[...].astype(f32)) * rate * learn_rate
    )
    new_gain = own_gain[...].reshape(1, share) - sum_vec[:, pl.ds(mine, share)]
    next_norm[...] = new_gain
    half_norm[:, pl.ds(mine, share)] = new_gain
    half_norm[:, pl.ds(theirs, share)] = (
        peer_gain[...].reshape(1, share) - sum_vec[:, pl.ds(theirs, share)]
    )

    ratio = jnp.sqrt(whole_norm(0)) * lax.rsqrt(whole_norm(2) + 1e-06)
    ratio = ratio * (rate * learn_rate)
    for c in range(up_chunks):
        spread[...] = jnp.broadcast_to(
            ratio[:, c * LANES : (c + 1) * LANES], (LANES, LANES)
        ).T

        @pl.loop(0, LANES // ROWS)
        def _(r):
            rows = pl.ds(c * LANES + r * ROWS, ROWS)
            scale = spread[pl.ds(r * ROWS, ROWS), :]
            for j in range(inner // LANES):
                lanes = pl.ds(j * LANES, LANES)
                new = next_up[rows, lanes] - sum_up(rows, lanes) * scale
                next_up[rows, lanes] = new
                half_up[pl.ds(mine + c * LANES + r * ROWS, ROWS), lanes] = new.astype(
                    jnp.bfloat16
                )

        block = half_up.at[pl.ds(mine + c * LANES, LANES), :]
        push(("half_up", c), block, block)

    ratio = jnp.sqrt(whole_norm(1)) * lax.rsqrt(whole_norm(3) + 1e-06)
    ratio = ratio * (rate * learn_rate)
    scales = [
        jnp.broadcast_to(ratio[:, j * LANES : (j + 1) * LANES], (ROWS, LANES))
        for j in range(share // LANES)
    ]
    for c in range(down_chunks):

        @pl.loop(0, down_rows // ROWS)
        def _(r):
            rows = pl.ds(c * down_rows + r * ROWS, ROWS)
            for j, scale in enumerate(scales):
                lanes = pl.ds(j * LANES, LANES)
                new = next_down[rows, lanes] - sum_down(rows, lanes) * scale
                next_down[rows, lanes] = new
                half_down[rows, pl.ds(mine + j * LANES, LANES)] = new.astype(
                    jnp.bfloat16
                )

        block = half_down.at[down_part(c), pl.ds(mine, share)]
        push(("half_down", c), block, block)

    for name, copy in pairs.items():
        copy.wait_send()
        if name[0] in ("half_up", "half_down"):
            copy.wait_recv()
    for _, copy in sent:
        copy.wait_send()


def write_kernel(
    half_up,
    half_down,
    half_norm,
    next_up,
    next_down,
    next_norm,
    half_up_out,
    half_down_out,
    half_norm_out,
    next_up_out,
    next_down_out,
    next_norm_out,
    sem,
):
    moves = (
        (half_up, half_up_out),
        (half_down, half_down_out),
        (next_up, next_up_out),
        (next_down, next_down_out),
    )
    copies = [
        pltpu.make_async_copy(source, target, sem.at[i])
        for i, (source, target) in enumerate(moves)
    ]
    for copy in copies:
        copy.start()
    half_norm_out[...] = half_norm[...].reshape(half_norm_out.shape).astype(
        jnp.bfloat16
    )
    next_norm_out[...] = next_norm[...].reshape(next_norm_out.shape)
    for copy in copies:
        copy.wait()


def fused(replicas, models, slope_up, slope_down, slope_norm, param_up, param_down, param_norm):
    share, inner = param_up.shape
    depth = param_down.shape[0]
    width = slope_up.shape[1]
    down_chunks = depth // (256 if depth % 256 == 0 else LANES)
    up_chunks = share // LANES
    moves = up_chunks + down_chunks + 2
    bf16, f32 = jnp.bfloat16, jnp.float32
    hbm = pl.BlockSpec(memory_space=pltpu.HBM)
    vmem = pl.BlockSpec(memory_space=pltpu.VMEM)
    outs = pl.pallas_call(
        functools.partial(update_kernel, replicas, models),
        out_shape=(
            OUT((width, inner), bf16),
            OUT((depth, width), bf16),
            OUT((1, width), f32),
            OUT((share, inner), f32),
            OUT((depth, share), f32),
            OUT((1, share), f32),
        ),
        in_specs=[hbm] * 6,
        out_specs=(vmem,) * 6,
        scratch_shapes=[
            pltpu.VMEM((share, inner), bf16),
            pltpu.VMEM((share, inner), bf16),
            pltpu.VMEM((depth, share), bf16),
            pltpu.VMEM((depth, share), bf16),
            pltpu.VMEM((1, width), bf16),
            pltpu.VMEM((1, width), bf16),
            pltpu.VMEM((share,), f32),
            pltpu.VMEM((share,), f32),
            pltpu.VMEM((1, width), f32),
            pltpu.VMEM((4, 1, share), f32),
            pltpu.VMEM((4, models - 1, 1, share), f32),
            pltpu.VMEM((LANES, LANES), f32),
            pltpu.VMEM((LANES, LANES), f32),
            pltpu.SemaphoreType.DMA((moves + 2,)),
            pltpu.SemaphoreType.DMA((2 * moves,)),
            pltpu.SemaphoreType.DMA((2 * moves,)),
            pltpu.SemaphoreType.DMA((4, models - 1)),
            pltpu.SemaphoreType.DMA((4, models - 1)),
        ],
        compiler_params=pltpu.CompilerParams(
            collective_id=0, has_side_effects=True, vmem_limit_bytes=24 * 2**20
        ),
    )(
        *(
            pltpu.with_memory_space_constraint(x, pltpu.HBM)
            for x in (
                slope_up, slope_down, slope_norm, param_up, param_down, param_norm
            )
        )
    )
    return pl.pallas_call(
        write_kernel,
        out_shape=(
            jax.ShapeDtypeStruct((width, inner), bf16),
            jax.ShapeDtypeStruct((depth, width), bf16),
            jax.ShapeDtypeStruct((width,), bf16),
            jax.ShapeDtypeStruct((share, inner), f32),
            jax.ShapeDtypeStruct((depth, share), f32),
            jax.ShapeDtypeStruct((share,), f32),
        ),
        in_specs=[vmem] * 6,
        out_specs=(hbm, hbm, vmem, hbm, hbm, vmem),
        scratch_shapes=[pltpu.SemaphoreType.DMA((4,))],
        compiler_params=pltpu.CompilerParams(vmem_limit_bytes=24 * 2**20),
    )(*(pltpu.with_memory_space_constraint(x, pltpu.VMEM) for x in outs))


def suits(mesh, *arrays):
    slope_up, param_up, param_down = arrays
    return (
        mesh.shape["replica"] == 2
        and mesh.shape["model"] > 1
        and param_up.shape[0] % LANES == 0
        and param_up.shape[1] % LANES == 0
        and param_down.shape[0] % LANES == 0
    )


def step(mesh, slope_up, slope_down, slope_norm, param_up, param_down, param_norm):
    args = (slope_up, slope_down, slope_norm, param_up, param_down, param_norm)
    if suits(mesh, slope_up, param_up, param_down):
        return fused(mesh.shape["replica"], mesh.shape["model"], *args)
    return shards(*args)


OUT = pltpu.VMEM


def solution(mesh):
    return jax.shard_map(
        functools.partial(step, mesh),
        mesh=mesh,
        in_specs=(
            P(("copy", "replica"), None, "model"),
            P(("copy", "replica"), "model", None),
            P(("copy", "replica"), None),
            P(("copy", "replica"), "model"),
            P(("copy", "model"), "replica"),
            P(("copy", "replica")),
        ),
        out_specs=(
            P("copy", "model"),
            P(("copy", "model"), None),
            P("copy"),
            P(("copy", "replica"), "model"),
            P(("copy", "model"), "replica"),
            P(("copy", "replica")),
        ),
        check_vma=False,
    )
```

```python
import functools

import jax
import jax.numpy as jnp
from jax import lax
from jax.experimental import pallas as pl
from jax.experimental.pallas import tpu as pltpu
from jax.sharding import PartitionSpec as P

learn_rate = 0.5


def shards(slope_up, slope_down, slope_norm, param_up, param_down, param_norm):
    mean_up, mean_down = (
        lax.psum_scatter(
            slope_up[0].astype(jnp.float32).astype(jnp.bfloat16),
            "replica",
            scatter_dimension=0,
            tiled=True,
        ).astype(jnp.float32),
        lax.psum_scatter(
            slope_down[0].astype(jnp.float32).astype(jnp.bfloat16),
            "replica",
            scatter_dimension=1,
            tiled=True,
        ).astype(jnp.float32),
    )
    whole_norm = lax.psum(slope_norm[0].astype(jnp.float32), "replica")
    place = lax.axis_index("replica")
    mean_norm = lax.dynamic_slice_in_dim(
        whole_norm, place * param_norm.shape[0], param_norm.shape[0]
    )
    mean_rate = lax.axis_size("replica") ** (-0.5)
    mean_up = mean_up * mean_rate
    mean_down = mean_down * mean_rate
    mean_norm = mean_norm * mean_rate
    own_up, own_down, slope_up_norm, slope_down_norm = lax.psum(
        (
            jnp.sum(param_up * param_up, axis=1, keepdims=True),
            jnp.sum(param_down * param_down, axis=0, keepdims=True),
            jnp.sum(mean_up * mean_up, axis=1, keepdims=True),
            jnp.sum(mean_down * mean_down, axis=0, keepdims=True),
        ),
        "model",
    )
    mean_up = mean_up * (jnp.sqrt(own_up) * lax.rsqrt(slope_up_norm + 1e-06))
    mean_down = mean_down * (jnp.sqrt(own_down) * lax.rsqrt(slope_down_norm + 1e-06))
    next_up = param_up - learn_rate * mean_up
    next_down = param_down - learn_rate * mean_down
    next_norm = param_norm - learn_rate * mean_norm
    half_up, half_down, half_norm = (
        lax.all_gather(next_up.astype(jnp.bfloat16), "replica", axis=0, tiled=True),
        lax.all_gather(next_down.astype(jnp.bfloat16), "replica", axis=1, tiled=True),
        lax.all_gather(next_norm.astype(jnp.bfloat16), "replica", axis=0, tiled=True),
    )
    return (half_up, half_down, half_norm, next_up, next_down, next_norm)


MESH = pl.DeviceIdType.MESH
LANES = 128
ROWS = 32
AHEAD = 6


def update_kernel(
    replicas,
    models,
    slope_up,
    slope_down,
    slope_norm,
    param_up,
    param_down,
    param_norm,
    half_up,
    half_down,
    half_norm,
    next_up,
    next_down,
    next_norm,
    own_up,
    peer_up,
    own_down,
    peer_down,
    own_vec,
    peer_vec,
    own_gain,
    peer_gain,
    sum_vec,
    part,
    got,
    piece,
    got_piece,
    square,
    spread,
    load_sem,
    pair_send,
    pair_recv,
    norm_send,
    norm_recv,
    piece_send,
    piece_recv,
):
    me = lax.axis_index("replica")
    other = 1 - me
    spot = lax.axis_index("model")
    share, inner = param_up.shape
    depth = param_down.shape[0]
    up_chunks = share // LANES
    down_chunks = share // LANES
    down_rows = 4 * ROWS
    mine = pl.multiple_of(me * share, LANES)
    theirs = pl.multiple_of(other * share, LANES)
    rate = replicas ** (-0.5)
    f32 = jnp.float32

    loads = {}

    def load(name, source, target):
        copy = pltpu.make_async_copy(source, target, load_sem.at[len(loads)])
        copy.start()
        loads[name] = copy

    pairs = {}

    def push(name, source, target):
        copy = pltpu.make_async_remote_copy(
            source,
            target,
            pair_send.at[len(pairs)],
            pair_recv.at[len(pairs)],
            device_id={"replica": other},
            device_id_type=MESH,
        )
        copy.start()
        pairs[name] = copy

    def up_rows(c):
        return pl.ds(c * LANES, LANES)

    def down_part(c):
        return pl.ds(c * LANES, LANES)

    load("pu", param_up, next_up)
    load("pd", param_down, next_down)
    for c in range(up_chunks):
        load(
            ("up", c),
            slope_up.at[0, pl.ds(mine + c * LANES, LANES), :],
            own_up.at[up_rows(c), :],
        )
    for c in range(down_chunks):
        load(
            ("down", c),
            slope_down.at[0, :, pl.ds(mine + c * LANES, LANES)],
            own_down.at[:, down_part(c)],
        )
    load("sn", slope_norm, own_vec)
    load("pn", param_norm, own_gain)

    barrier = pltpu.get_barrier_semaphore()
    pl.semaphore_signal(
        barrier, inc=1, device_id={"replica": other}, device_id_type=MESH
    )
    for k in range(1, models):
        pl.semaphore_signal(
            barrier,
            inc=1,
            device_id={"model": lax.rem(spot + k, models)},
            device_id_type=MESH,
        )
    pl.semaphore_wait(barrier, models)

    for c in range(up_chunks):
        push(
            ("up", c),
            slope_up.at[0, pl.ds(theirs + c * LANES, LANES), :],
            peer_up.at[up_rows(c), :],
        )
    for c in range(down_chunks):
        push(
            ("down", c),
            slope_down.at[0, :, pl.ds(theirs + c * LANES, LANES)],
            peer_down.at[:, down_part(c)],
        )
    push("sn", slope_norm, peer_vec)
    push("pn", param_norm, peer_gain)

    sent = []

    def share_norm(source, target, sems, i):
        copies = []
        for k in range(1, models):
            copy = pltpu.make_async_remote_copy(
                source.at[i],
                target.at[i, k - 1],
                sems[0].at[i, k - 1],
                sems[1].at[i, k - 1],
                device_id={"model": lax.rem(spot + k, models)},
                device_id_type=MESH,
            )
            copy.start()
            copies.append(copy)
        sent.extend(copies)

        def whole():
            for copy in copies:
                copy.wait_recv()
            total = source[i]
            for k in range(1, models):
                total = total + target[i, k - 1]
            return total

        return whole

    def share_param(i):
        return share_norm(part, got, (norm_send, norm_recv), i)

    def share_slope(i):
        return share_norm(piece, got_piece, (piece_send, piece_recv), i)

    def row_squares(c, value):
        @pl.loop(0, LANES // ROWS)
        def _(r):
            rows = pl.ds(c * LANES + r * ROWS, ROWS)
            total = jnp.zeros((ROWS, LANES), f32)
            for j in range(inner // LANES):
                x = value(rows, pl.ds(j * LANES, LANES))
                total = total + x * x
            square[pl.ds(r * ROWS, ROWS), :] = total

        return jnp.sum(square[...].T, axis=0, keepdims=True)

    def column_squares(c, value):
        def body(r, total):
            for q in range(down_rows // ROWS):
                x = value(pl.ds(r * down_rows + q * ROWS, ROWS), down_part(c))
                total = total + x * x
            return total

        total = lax.fori_loop(
            0, depth // down_rows, body, jnp.zeros((ROWS, LANES), f32)
        )
        return jnp.sum(total, axis=0, keepdims=True)

    def sum_up(rows, lanes):
        return own_up[rows, lanes].astype(f32) + peer_up[rows, lanes].astype(f32)

    def sum_down(rows, lanes):
        return own_down[rows, lanes].astype(f32) + peer_down[rows, lanes].astype(f32)

    loads["pu"].wait()
    for c in range(up_chunks):
        part[0, :, c * LANES : (c + 1) * LANES] = row_squares(
            c, lambda rows, lanes: next_up[rows, lanes]
        )
    whole_up = share_param(0)
    loads["pd"].wait()
    for c in range(down_chunks):
        part[1, :, c * LANES : (c + 1) * LANES] = column_squares(
            c, lambda rows, lanes: next_down[rows, lanes]
        )
    whole_down = share_param(1)

    pieces = [("up", c) for c in range(up_chunks)]
    pieces += [("down", c) for c in range(down_chunks)]
    slope_wholes = {}
    param_wholes = {}

    def measure_piece(n):
        kind, c = pieces[n]
        loads[pieces[n]].wait()
        pairs[pieces[n]].wait_recv()
        if kind == "up":
            piece[n] = row_squares(c, lambda rows, lanes: sum_up(rows, lanes) * rate)
        else:
            piece[n] = column_squares(
                c, lambda rows, lanes: sum_down(rows, lanes) * rate
            )
        slope_wholes[n] = share_slope(n)

    def update_piece(n):
        kind, c = pieces[n]
        if kind not in param_wholes:
            total = (whole_up if kind == "up" else whole_down)()
            param_wholes[kind] = jnp.sqrt(total) * (rate * learn_rate)
        ratio = param_wholes[kind][:, c * LANES : (c + 1) * LANES] * lax.rsqrt(
            slope_wholes[n]() + 1e-06
        )
        if kind == "up":
            update_up(c, ratio)
        else:
            update_down(c, ratio)

    def update_up(c, ratio):
        spread[...] = jnp.broadcast_to(ratio, (LANES, LANES)).T

        @pl.loop(0, LANES // ROWS)
        def _(r):
            rows = pl.ds(c * LANES + r * ROWS, ROWS)
            scale = spread[pl.ds(r * ROWS, ROWS), :]
            for j in range(inner // LANES):
                lanes = pl.ds(j * LANES, LANES)
                new = next_up[rows, lanes] - sum_up(rows, lanes) * scale
                next_up[rows, lanes] = new
                half_up[pl.ds(mine + c * LANES + r * ROWS, ROWS), lanes] = new.astype(
                    jnp.bfloat16
                )

        block = half_up.at[pl.ds(mine + c * LANES, LANES), :]
        push(("half_up", c), block, block)

    def update_down(c, ratio):
        scale = jnp.broadcast_to(ratio, (ROWS, LANES))
        lanes = down_part(c)
        place = pl.ds(mine + c * LANES, LANES)

        @pl.loop(0, depth // down_rows)
        def _(r):
            for q in range(down_rows // ROWS):
                rows = pl.ds(r * down_rows + q * ROWS, ROWS)
                new = next_down[rows, lanes] - sum_down(rows, lanes) * scale
                next_down[rows, lanes] = new
                half_down[rows, place] = new.astype(jnp.bfloat16)

        block = half_down.at[:, place]
        push(("half_down", c), block, block)

    ahead = min(AHEAD, len(pieces))
    for n in range(len(pieces) + ahead):
        if n < len(pieces):
            measure_piece(n)
        if n >= ahead:
            update_piece(n - ahead)

    loads["sn"].wait()
    loads["pn"].wait()
    pairs["sn"].wait_recv()
    pairs["pn"].wait_recv()
    sum_vec[...] = (
        (own_vec[...].astype(f32) + peer_vec[...].astype(f32)) * rate * learn_rate
    )
    new_gain = own_gain[...].reshape(1, share) - sum_vec[:, pl.ds(mine, share)]
    next_norm[...] = new_gain
    half_norm[:, pl.ds(mine, share)] = new_gain
    half_norm[:, pl.ds(theirs, share)] = (
        peer_gain[...].reshape(1, share) - sum_vec[:, pl.ds(theirs, share)]
    )

    for name, copy in pairs.items():
        copy.wait_send()
        if name[0] in ("half_up", "half_down"):
            copy.wait_recv()
    for copy in sent:
        copy.wait_send()


def write_kernel(
    half_up,
    half_down,
    half_norm,
    next_up,
    next_down,
    next_norm,
    half_up_out,
    half_down_out,
    half_norm_out,
    next_up_out,
    next_down_out,
    next_norm_out,
    sem,
):
    moves = (
        (half_up, half_up_out),
        (half_down, half_down_out),
        (next_up, next_up_out),
        (next_down, next_down_out),
    )
    copies = [
        pltpu.make_async_copy(source, target, sem.at[i])
        for i, (source, target) in enumerate(moves)
    ]
    for copy in copies:
        copy.start()
    half_norm_out[...] = half_norm[...].reshape(half_norm_out.shape).astype(
        jnp.bfloat16
    )
    next_norm_out[...] = next_norm[...].reshape(next_norm_out.shape)
    for copy in copies:
        copy.wait()


def fused(replicas, models, slope_up, slope_down, slope_norm, param_up, param_down, param_norm):
    share, inner = param_up.shape
    depth = param_down.shape[0]
    width = slope_up.shape[1]
    down_chunks = share // LANES
    up_chunks = share // LANES
    moves = up_chunks + down_chunks + 2
    bf16, f32 = jnp.bfloat16, jnp.float32
    hbm = pl.BlockSpec(memory_space=pltpu.HBM)
    vmem = pl.BlockSpec(memory_space=pltpu.VMEM)
    outs = pl.pallas_call(
        functools.partial(update_kernel, replicas, models),
        out_shape=(
            OUT((width, inner), bf16),
            OUT((depth, width), bf16),
            OUT((1, width), f32),
            OUT((share, inner), f32),
            OUT((depth, share), f32),
            OUT((1, share), f32),
        ),
        in_specs=[hbm] * 6,
        out_specs=(vmem,) * 6,
        scratch_shapes=[
            pltpu.VMEM((share, inner), bf16),
            pltpu.VMEM((share, inner), bf16),
            pltpu.VMEM((depth, share), bf16),
            pltpu.VMEM((depth, share), bf16),
            pltpu.VMEM((1, width), bf16),
            pltpu.VMEM((1, width), bf16),
            pltpu.VMEM((share,), f32),
            pltpu.VMEM((share,), f32),
            pltpu.VMEM((1, width), f32),
            pltpu.VMEM((2, 1, share), f32),
            pltpu.VMEM((2, models - 1, 1, share), f32),
            pltpu.VMEM((moves - 2, 1, LANES), f32),
            pltpu.VMEM((moves - 2, models - 1, 1, LANES), f32),
            pltpu.VMEM((LANES, LANES), f32),
            pltpu.VMEM((LANES, LANES), f32),
            pltpu.SemaphoreType.DMA((moves + 2,)),
            pltpu.SemaphoreType.DMA((2 * moves,)),
            pltpu.SemaphoreType.DMA((2 * moves,)),
            pltpu.SemaphoreType.DMA((2, models - 1)),
            pltpu.SemaphoreType.DMA((2, models - 1)),
            pltpu.SemaphoreType.DMA((moves - 2, models - 1)),
            pltpu.SemaphoreType.DMA((moves - 2, models - 1)),
        ],
        compiler_params=pltpu.CompilerParams(
            collective_id=0, has_side_effects=True, vmem_limit_bytes=24 * 2**20
        ),
    )(
        *(
            pltpu.with_memory_space_constraint(x, pltpu.HBM)
            for x in (
                slope_up, slope_down, slope_norm, param_up, param_down, param_norm
            )
        )
    )
    return pl.pallas_call(
        write_kernel,
        out_shape=(
            jax.ShapeDtypeStruct((width, inner), bf16),
            jax.ShapeDtypeStruct((depth, width), bf16),
            jax.ShapeDtypeStruct((width,), bf16),
            jax.ShapeDtypeStruct((share, inner), f32),
            jax.ShapeDtypeStruct((depth, share), f32),
            jax.ShapeDtypeStruct((share,), f32),
        ),
        in_specs=[vmem] * 6,
        out_specs=(hbm, hbm, vmem, hbm, hbm, vmem),
        scratch_shapes=[pltpu.SemaphoreType.DMA((4,))],
        compiler_params=pltpu.CompilerParams(vmem_limit_bytes=24 * 2**20),
    )(*(pltpu.with_memory_space_constraint(x, pltpu.VMEM) for x in outs))


def suits(mesh, *arrays):
    slope_up, param_up, param_down = arrays
    return (
        mesh.shape["replica"] == 2
        and mesh.shape["model"] > 1
        and param_up.shape[0] % LANES == 0
        and param_up.shape[1] % LANES == 0
        and param_down.shape[0] % LANES == 0
    )


def step(mesh, slope_up, slope_down, slope_norm, param_up, param_down, param_norm):
    args = (slope_up, slope_down, slope_norm, param_up, param_down, param_norm)
    if suits(mesh, slope_up, param_up, param_down):
        return fused(mesh.shape["replica"], mesh.shape["model"], *args)
    return shards(*args)


OUT = pltpu.VMEM


def solution(mesh):
    return jax.shard_map(
        functools.partial(step, mesh),
        mesh=mesh,
        in_specs=(
            P(("copy", "replica"), None, "model"),
            P(("copy", "replica"), "model", None),
            P(("copy", "replica"), None),
            P(("copy", "replica"), "model"),
            P(("copy", "model"), "replica"),
            P(("copy", "replica")),
        ),
        out_specs=(
            P("copy", "model"),
            P(("copy", "model"), None),
            P("copy"),
            P(("copy", "replica"), "model"),
            P(("copy", "model"), "replica"),
            P(("copy", "replica")),
        ),
        check_vma=False,
    )
```

```python
import functools

import jax
import jax.numpy as jnp
from jax import lax
from jax.experimental import pallas as pl
from jax.experimental.pallas import tpu as pltpu
from jax.sharding import PartitionSpec as P

learn_rate = 0.5


def shards(slope_up, slope_down, slope_norm, param_up, param_down, param_norm):
    mean_up, mean_down = (
        lax.psum_scatter(
            slope_up[0].astype(jnp.float32).astype(jnp.bfloat16),
            "replica",
            scatter_dimension=0,
            tiled=True,
        ).astype(jnp.float32),
        lax.psum_scatter(
            slope_down[0].astype(jnp.float32).astype(jnp.bfloat16),
            "replica",
            scatter_dimension=1,
            tiled=True,
        ).astype(jnp.float32),
    )
    whole_norm = lax.psum(slope_norm[0].astype(jnp.float32), "replica")
    place = lax.axis_index("replica")
    mean_norm = lax.dynamic_slice_in_dim(
        whole_norm, place * param_norm.shape[0], param_norm.shape[0]
    )
    mean_rate = lax.axis_size("replica") ** (-0.5)
    mean_up = mean_up * mean_rate
    mean_down = mean_down * mean_rate
    mean_norm = mean_norm * mean_rate
    own_up, own_down, slope_up_norm, slope_down_norm = lax.psum(
        (
            jnp.sum(param_up * param_up, axis=1, keepdims=True),
            jnp.sum(param_down * param_down, axis=0, keepdims=True),
            jnp.sum(mean_up * mean_up, axis=1, keepdims=True),
            jnp.sum(mean_down * mean_down, axis=0, keepdims=True),
        ),
        "model",
    )
    mean_up = mean_up * (jnp.sqrt(own_up) * lax.rsqrt(slope_up_norm + 1e-06))
    mean_down = mean_down * (jnp.sqrt(own_down) * lax.rsqrt(slope_down_norm + 1e-06))
    next_up = param_up - learn_rate * mean_up
    next_down = param_down - learn_rate * mean_down
    next_norm = param_norm - learn_rate * mean_norm
    half_up, half_down, half_norm = (
        lax.all_gather(next_up.astype(jnp.bfloat16), "replica", axis=0, tiled=True),
        lax.all_gather(next_down.astype(jnp.bfloat16), "replica", axis=1, tiled=True),
        lax.all_gather(next_norm.astype(jnp.bfloat16), "replica", axis=0, tiled=True),
    )
    return (half_up, half_down, half_norm, next_up, next_down, next_norm)


MESH = pl.DeviceIdType.MESH
LANES = 128
ROWS = 32
AHEAD = 6


def update_kernel(
    replicas,
    models,
    slope_up,
    slope_down,
    slope_norm,
    param_up,
    param_down,
    param_norm,
    half_up,
    half_down,
    half_norm,
    next_up,
    next_down,
    next_norm,
    own_up,
    peer_up,
    own_down,
    peer_down,
    own_vec,
    peer_vec,
    own_gain,
    peer_gain,
    sum_vec,
    part,
    got,
    piece,
    got_piece,
    square,
    spread,
    load_sem,
    pair_send,
    pair_recv,
    norm_send,
    norm_recv,
    piece_send,
    piece_recv,
):
    me = lax.axis_index("replica")
    other = 1 - me
    spot = lax.axis_index("model")
    share, inner = param_up.shape
    depth = param_down.shape[0]
    up_chunks = share // LANES
    down_chunks = share // LANES
    down_rows = 4 * ROWS
    mine = pl.multiple_of(me * share, LANES)
    theirs = pl.multiple_of(other * share, LANES)
    rate = replicas ** (-0.5)
    f32 = jnp.float32

    loads = {}

    def load(name, source, target):
        copy = pltpu.make_async_copy(source, target, load_sem.at[len(loads)])
        copy.start()
        loads[name] = copy

    pairs = {}

    def push(name, source, target):
        copy = pltpu.make_async_remote_copy(
            source,
            target,
            pair_send.at[len(pairs)],
            pair_recv.at[len(pairs)],
            device_id={"replica": other},
            device_id_type=MESH,
        )
        copy.start()
        pairs[name] = copy

    def up_rows(c):
        return pl.ds(c * LANES, LANES)

    def down_part(c):
        return pl.ds(c * LANES, LANES)

    load("pu", param_up, next_up)
    load("pd", param_down, next_down)
    for c in range(up_chunks):
        load(
            ("up", c),
            slope_up.at[0, pl.ds(mine + c * LANES, LANES), :],
            own_up.at[up_rows(c), :],
        )
    for c in range(down_chunks):
        load(
            ("down", c),
            slope_down.at[0, :, pl.ds(mine + c * LANES, LANES)],
            own_down.at[:, down_part(c)],
        )
    load("sn", slope_norm, own_vec)
    load("pn", param_norm, own_gain)

    barrier = pltpu.get_barrier_semaphore()
    pl.semaphore_signal(
        barrier, inc=1, device_id={"replica": other}, device_id_type=MESH
    )
    for k in range(1, models):
        pl.semaphore_signal(
            barrier,
            inc=1,
            device_id={"model": lax.rem(spot + k, models)},
            device_id_type=MESH,
        )
    pl.semaphore_wait(barrier, models)

    for c in range(up_chunks):
        push(
            ("up", c),
            slope_up.at[0, pl.ds(theirs + c * LANES, LANES), :],
            peer_up.at[up_rows(c), :],
        )
    for c in range(down_chunks):
        push(
            ("down", c),
            slope_down.at[0, :, pl.ds(theirs + c * LANES, LANES)],
            peer_down.at[:, down_part(c)],
        )
    push("sn", slope_norm, peer_vec)
    push("pn", param_norm, peer_gain)

    sent = []

    def share_norm(source, target, sems, i):
        copies = []
        for k in range(1, models):
            copy = pltpu.make_async_remote_copy(
                source.at[i],
                target.at[i, k - 1],
                sems[0].at[i, k - 1],
                sems[1].at[i, k - 1],
                device_id={"model": lax.rem(spot + k, models)},
                device_id_type=MESH,
            )
            copy.start()
            copies.append(copy)
        sent.extend(copies)

        def whole():
            for copy in copies:
                copy.wait_recv()
            total = source[i]
            for k in range(1, models):
                total = total + target[i, k - 1]
            return total

        return whole

    def share_param(i):
        return share_norm(part, got, (norm_send, norm_recv), i)

    def share_slope(i):
        return share_norm(piece, got_piece, (piece_send, piece_recv), i)

    def row_squares(c, value):
        @pl.loop(0, LANES // ROWS)
        def _(r):
            rows = pl.ds(c * LANES + r * ROWS, ROWS)
            total = jnp.zeros((ROWS, LANES), f32)
            for j in range(inner // LANES):
                x = value(rows, pl.ds(j * LANES, LANES))
                total = total + x * x
            square[pl.ds(r * ROWS, ROWS), :] = total

        return jnp.sum(square[...].T, axis=0, keepdims=True)

    def column_squares(c, value):
        def body(r, total):
            for q in range(down_rows // ROWS):
                x = value(pl.ds(r * down_rows + q * ROWS, ROWS), down_part(c))
                total = total + x * x
            return total

        total = lax.fori_loop(
            0, depth // down_rows, body, jnp.zeros((ROWS, LANES), f32)
        )
        return jnp.sum(total, axis=0, keepdims=True)

    def sum_up(rows, lanes):
        return own_up[rows, lanes].astype(f32) + peer_up[rows, lanes].astype(f32)

    def sum_down(rows, lanes):
        return own_down[rows, lanes].astype(f32) + peer_down[rows, lanes].astype(f32)

    loads["pu"].wait()
    for c in range(up_chunks):
        part[0, :, c * LANES : (c + 1) * LANES] = row_squares(
            c, lambda rows, lanes: next_up[rows, lanes]
        )
    whole_up = share_param(0)

    def measure_down():
        loads["pd"].wait()
        for c in range(down_chunks):
            part[1, :, c * LANES : (c + 1) * LANES] = column_squares(
                c, lambda rows, lanes: next_down[rows, lanes]
            )
        return share_param(1)

    pieces = [("up", c) for c in range(up_chunks)]
    pieces += [("down", c) for c in range(down_chunks)]
    slope_wholes = {}
    param_wholes = {}

    def measure_piece(n):
        kind, c = pieces[n]
        loads[pieces[n]].wait()
        pairs[pieces[n]].wait_recv()
        if kind == "up":
            piece[n] = row_squares(c, lambda rows, lanes: sum_up(rows, lanes) * rate)
        else:
            piece[n] = column_squares(
                c, lambda rows, lanes: sum_down(rows, lanes) * rate
            )
        slope_wholes[n] = share_slope(n)

    def update_piece(n):
        kind, c = pieces[n]
        if kind not in param_wholes:
            total = (whole_up if kind == "up" else whole_down)()
            param_wholes[kind] = jnp.sqrt(total) * (rate * learn_rate)
        ratio = param_wholes[kind][:, c * LANES : (c + 1) * LANES] * lax.rsqrt(
            slope_wholes[n]() + 1e-06
        )
        if kind == "up":
            update_up(c, ratio)
        else:
            update_down(c, ratio)

    def update_up(c, ratio):
        spread[...] = jnp.broadcast_to(ratio, (LANES, LANES)).T

        @pl.loop(0, LANES // ROWS)
        def _(r):
            rows = pl.ds(c * LANES + r * ROWS, ROWS)
            scale = spread[pl.ds(r * ROWS, ROWS), :]
            for j in range(inner // LANES):
                lanes = pl.ds(j * LANES, LANES)
                new = next_up[rows, lanes] - sum_up(rows, lanes) * scale
                next_up[rows, lanes] = new
                half_up[pl.ds(mine + c * LANES + r * ROWS, ROWS), lanes] = new.astype(
                    jnp.bfloat16
                )

        block = half_up.at[pl.ds(mine + c * LANES, LANES), :]
        push(("half_up", c), block, block)

    def update_down(c, ratio):
        scale = jnp.broadcast_to(ratio, (ROWS, LANES))
        lanes = down_part(c)
        place = pl.ds(mine + c * LANES, LANES)

        @pl.loop(0, depth // down_rows)
        def _(r):
            for q in range(down_rows // ROWS):
                rows = pl.ds(r * down_rows + q * ROWS, ROWS)
                new = next_down[rows, lanes] - sum_down(rows, lanes) * scale
                next_down[rows, lanes] = new
                half_down[rows, place] = new.astype(jnp.bfloat16)

        block = half_down.at[:, place]
        push(("half_down", c), block, block)

    ahead = min(AHEAD, len(pieces))
    for n in range(len(pieces) + ahead):
        if n == 2:
            whole_down = measure_down()
        if n < len(pieces):
            measure_piece(n)
        if n >= ahead:
            update_piece(n - ahead)

    loads["sn"].wait()
    loads["pn"].wait()
    pairs["sn"].wait_recv()
    pairs["pn"].wait_recv()
    sum_vec[...] = (
        (own_vec[...].astype(f32) + peer_vec[...].astype(f32)) * rate * learn_rate
    )
    new_gain = own_gain[...].reshape(1, share) - sum_vec[:, pl.ds(mine, share)]
    next_norm[...] = new_gain
    half_norm[:, pl.ds(mine, share)] = new_gain
    half_norm[:, pl.ds(theirs, share)] = (
        peer_gain[...].reshape(1, share) - sum_vec[:, pl.ds(theirs, share)]
    )

    for name, copy in pairs.items():
        copy.wait_send()
        if name[0] in ("half_up", "half_down"):
            copy.wait_recv()
    for copy in sent:
        copy.wait_send()


def write_kernel(
    half_up,
    half_down,
    half_norm,
    next_up,
    next_down,
    next_norm,
    half_up_out,
    half_down_out,
    half_norm_out,
    next_up_out,
    next_down_out,
    next_norm_out,
    sem,
):
    moves = (
        (half_up, half_up_out),
        (half_down, half_down_out),
        (next_up, next_up_out),
        (next_down, next_down_out),
    )
    copies = [
        pltpu.make_async_copy(source, target, sem.at[i])
        for i, (source, target) in enumerate(moves)
    ]
    for copy in copies:
        copy.start()
    half_norm_out[...] = half_norm[...].reshape(half_norm_out.shape).astype(
        jnp.bfloat16
    )
    next_norm_out[...] = next_norm[...].reshape(next_norm_out.shape)
    for copy in copies:
        copy.wait()


def fused(replicas, models, slope_up, slope_down, slope_norm, param_up, param_down, param_norm):
    share, inner = param_up.shape
    depth = param_down.shape[0]
    width = slope_up.shape[1]
    down_chunks = share // LANES
    up_chunks = share // LANES
    moves = up_chunks + down_chunks + 2
    bf16, f32 = jnp.bfloat16, jnp.float32
    hbm = pl.BlockSpec(memory_space=pltpu.HBM)
    vmem = pl.BlockSpec(memory_space=pltpu.VMEM)
    outs = pl.pallas_call(
        functools.partial(update_kernel, replicas, models),
        out_shape=(
            OUT((width, inner), bf16),
            OUT((depth, width), bf16),
            OUT((1, width), f32),
            OUT((share, inner), f32),
            OUT((depth, share), f32),
            OUT((1, share), f32),
        ),
        in_specs=[hbm] * 6,
        out_specs=(vmem,) * 6,
        scratch_shapes=[
            pltpu.VMEM((share, inner), bf16),
            pltpu.VMEM((share, inner), bf16),
            pltpu.VMEM((depth, share), bf16),
            pltpu.VMEM((depth, share), bf16),
            pltpu.VMEM((1, width), bf16),
            pltpu.VMEM((1, width), bf16),
            pltpu.VMEM((share,), f32),
            pltpu.VMEM((share,), f32),
            pltpu.VMEM((1, width), f32),
            pltpu.VMEM((2, 1, share), f32),
            pltpu.VMEM((2, models - 1, 1, share), f32),
            pltpu.VMEM((moves - 2, 1, LANES), f32),
            pltpu.VMEM((moves - 2, models - 1, 1, LANES), f32),
            pltpu.VMEM((LANES, LANES), f32),
            pltpu.VMEM((LANES, LANES), f32),
            pltpu.SemaphoreType.DMA((moves + 2,)),
            pltpu.SemaphoreType.DMA((2 * moves,)),
            pltpu.SemaphoreType.DMA((2 * moves,)),
            pltpu.SemaphoreType.DMA((2, models - 1)),
            pltpu.SemaphoreType.DMA((2, models - 1)),
            pltpu.SemaphoreType.DMA((moves - 2, models - 1)),
            pltpu.SemaphoreType.DMA((moves - 2, models - 1)),
        ],
        compiler_params=pltpu.CompilerParams(
            collective_id=0, has_side_effects=True, vmem_limit_bytes=24 * 2**20
        ),
    )(
        *(
            pltpu.with_memory_space_constraint(x, pltpu.HBM)
            for x in (
                slope_up, slope_down, slope_norm, param_up, param_down, param_norm
            )
        )
    )
    return pl.pallas_call(
        write_kernel,
        out_shape=(
            jax.ShapeDtypeStruct((width, inner), bf16),
            jax.ShapeDtypeStruct((depth, width), bf16),
            jax.ShapeDtypeStruct((width,), bf16),
            jax.ShapeDtypeStruct((share, inner), f32),
            jax.ShapeDtypeStruct((depth, share), f32),
            jax.ShapeDtypeStruct((share,), f32),
        ),
        in_specs=[vmem] * 6,
        out_specs=(hbm, hbm, vmem, hbm, hbm, vmem),
        scratch_shapes=[pltpu.SemaphoreType.DMA((4,))],
        compiler_params=pltpu.CompilerParams(vmem_limit_bytes=24 * 2**20),
    )(*(pltpu.with_memory_space_constraint(x, pltpu.VMEM) for x in outs))


def suits(mesh, *arrays):
    slope_up, param_up, param_down = arrays
    return (
        mesh.shape["replica"] == 2
        and mesh.shape["model"] > 1
        and param_up.shape[0] % LANES == 0
        and param_up.shape[1] % LANES == 0
        and param_down.shape[0] % LANES == 0
    )


def step(mesh, slope_up, slope_down, slope_norm, param_up, param_down, param_norm):
    args = (slope_up, slope_down, slope_norm, param_up, param_down, param_norm)
    if suits(mesh, slope_up, param_up, param_down):
        return fused(mesh.shape["replica"], mesh.shape["model"], *args)
    return shards(*args)


OUT = pltpu.VMEM


def solution(mesh):
    return jax.shard_map(
        functools.partial(step, mesh),
        mesh=mesh,
        in_specs=(
            P(("copy", "replica"), None, "model"),
            P(("copy", "replica"), "model", None),
            P(("copy", "replica"), None),
            P(("copy", "replica"), "model"),
            P(("copy", "model"), "replica"),
            P(("copy", "replica")),
        ),
        out_specs=(
            P("copy", "model"),
            P(("copy", "model"), None),
            P("copy"),
            P(("copy", "replica"), "model"),
            P(("copy", "model"), "replica"),
            P(("copy", "replica")),
        ),
        check_vma=False,
    )
```
